32 devices in a mesh: dp: 1 (over z), sp: 32 (over y, x, core).
Axes of the slice: x: 4, y: 4, z: 1, core: 2. Of those that a mesh axis runs over, the one named last changes fastest.
The devices are a block of a 4x4x8 slice.
Arguments:
- latents: bfloat16 [6, 64, 256, 384], P('dp', 'sp')
- text_ctx: bfloat16 [6, 120, 384], P('dp')
- modulation: float32 [6, 6, 384], P('dp')
- pos_temporal: float32 [64, 384], replicated
- w_qkv_spatial: bfloat16 [3, 6, 64, 384], replicated
- w_out_spatial: bfloat16 [6, 64, 384], replicated
- w_qkv_temporal: bfloat16 [3, 6, 64, 384], replicated
- w_out_temporal: bfloat16 [6, 64, 384], replicated
- w_query_cross: bfloat16 [6, 64, 384], replicated
- w_kv_cross: bfloat16 [2, 6, 64, 384], replicated
- w_out_cross: bfloat16 [6, 64, 384], replicated
- w_mlp_in: bfloat16 [384, 1536], replicated
- w_mlp_out: bfloat16 [1536, 384], replicated
Outputs:
- output: bfloat16 [6, 64, 256, 384], P('dp', 'sp')
All inputs are finite; a program needn't handle non-finite values.
Results may differ from the reference program's by a relative error of at most 0.014326.
Values are sent between devices in bfloat16 or wider.
A program may use at most 768 MiB of HBM per device.

```python
import jax
import jax.numpy as jnp
from jax import lax

BATCH_SIZE = 6
NUM_FRAMES = 64
NUM_PATCHES = 256
MODEL_WIDTH = 384
NUM_HEADS = 6
TEXT_LEN = 120

HEAD_DIM = MODEL_WIDTH // NUM_HEADS
LN_EPS = 1e-6


def weight_draw(rng_key, arr_shape, fan_in):
    return (jax.random.normal(rng_key, arr_shape, jnp.float32) * (fan_in ** -0.5)).astype(jnp.bfloat16)


def setup_inputs(seed: int = 0, part: int = 0) -> dict:
    part_keys = jax.random.split(jax.random.fold_in(jax.random.key(seed), part), 6)
    shared_keys = jax.random.split(jax.random.key(seed + 1), 11)
    act_shape = (BATCH_SIZE, NUM_FRAMES, NUM_PATCHES, MODEL_WIDTH)
    token_base = jax.random.normal(part_keys[0], (BATCH_SIZE, 1, NUM_PATCHES, MODEL_WIDTH), jnp.float32)
    frame_base = jax.random.normal(part_keys[1], (BATCH_SIZE, NUM_FRAMES, 1, MODEL_WIDTH), jnp.float32)
    noise_part = jax.random.normal(part_keys[2], act_shape, jnp.float32)
    latents = (0.5 * token_base + 0.5 * frame_base + 0.6 * noise_part).astype(jnp.bfloat16)
    ctx_common = jax.random.normal(part_keys[3], (BATCH_SIZE, 1, MODEL_WIDTH), jnp.float32)
    ctx_noise = jax.random.normal(part_keys[4], (BATCH_SIZE, TEXT_LEN, MODEL_WIDTH), jnp.float32)
    text_ctx = (0.5 * ctx_common + ctx_noise).astype(jnp.bfloat16)
    gate_offset = jnp.array([0.0, 0.0, 1.0, 0.0, 0.0, 1.0], jnp.float32)[None, :, None]
    modulation = 0.3 * jax.random.normal(part_keys[5], (BATCH_SIZE, 6, MODEL_WIDTH), jnp.float32) + gate_offset
    pos_common = jax.random.normal(shared_keys[0], (1, MODEL_WIDTH), jnp.float32)
    pos_frames = jax.random.normal(shared_keys[1], (NUM_FRAMES, MODEL_WIDTH), jnp.float32)
    pos_temporal = 0.4 * pos_common + 0.4 * pos_frames
    head_shape = (NUM_HEADS, HEAD_DIM, MODEL_WIDTH)
    return {
        'latents': latents,
        'text_ctx': text_ctx,
        'modulation': modulation,
        'pos_temporal': pos_temporal,
        'w_qkv_spatial': weight_draw(shared_keys[2], (3,) + head_shape, MODEL_WIDTH),
        'w_out_spatial': weight_draw(shared_keys[3], head_shape, MODEL_WIDTH),
        'w_qkv_temporal': weight_draw(shared_keys[4], (3,) + head_shape, MODEL_WIDTH),
        'w_out_temporal': weight_draw(shared_keys[5], head_shape, MODEL_WIDTH),
        'w_query_cross': weight_draw(shared_keys[6], head_shape, MODEL_WIDTH),
        'w_kv_cross': weight_draw(shared_keys[7], (2,) + head_shape, MODEL_WIDTH),
        'w_out_cross': weight_draw(shared_keys[8], head_shape, MODEL_WIDTH),
        'w_mlp_in': weight_draw(shared_keys[9], (MODEL_WIDTH, 4 * MODEL_WIDTH), MODEL_WIDTH),
        'w_mlp_out': weight_draw(shared_keys[10], (4 * MODEL_WIDTH, MODEL_WIDTH), 4 * MODEL_WIDTH),
    }


def layer_norm(acts_in):
    centered = acts_in - jnp.mean(acts_in, axis=-1, keepdims=True)
    return centered * lax.rsqrt(jnp.mean(centered * centered, axis=-1, keepdims=True) + LN_EPS)


def attend(query_heads, key_heads, value_heads):
    scores = jnp.einsum('bqhd,bkhd->bhqk', query_heads.astype(jnp.float32), key_heads.astype(jnp.float32))
    attn_probs = jax.nn.softmax(scores * (HEAD_DIM ** -0.5), axis=-1).astype(jnp.bfloat16)
    mixed_out = jnp.einsum('bhqk,bkhd->bqhd', attn_probs.astype(jnp.float32), value_heads.astype(jnp.float32))
    return mixed_out.astype(jnp.bfloat16)


def qkv_proj(acts_in, weight):
    return jnp.einsum('bnc,jhdc->jbnhd', acts_in.astype(jnp.float32), weight.astype(jnp.float32)).astype(jnp.bfloat16)


def out_proj(mixed_in, weight):
    return jnp.einsum('bnhd,hdc->bnc', mixed_in.astype(jnp.float32), weight.astype(jnp.float32))


def reference(latents, text_ctx, modulation, pos_temporal, w_qkv_spatial, w_out_spatial, w_qkv_temporal, w_out_temporal, w_query_cross, w_kv_cross, w_out_cross, w_mlp_in, w_mlp_out):
    mod_rows = jnp.moveaxis(modulation, 1, 0)[:, :, None, :]

    def spatial_frame(frame_in):
        frame_f = frame_in.astype(jnp.float32)
        normed = (layer_norm(frame_f) * (1.0 + mod_rows[1]) + mod_rows[0]).astype(jnp.bfloat16)
        qkv_all = qkv_proj(normed, w_qkv_spatial)
        mixed_out = attend(qkv_all[0], qkv_all[1], qkv_all[2])
        return (frame_f + mod_rows[2] * out_proj(mixed_out, w_out_spatial)).astype(jnp.bfloat16)

    def temporal_patch(column_in):
        column_f = column_in.astype(jnp.float32)
        shifted = (column_f + pos_temporal[None]).astype(jnp.bfloat16)
        qkv_all = qkv_proj(shifted, w_qkv_temporal)
        mixed_out = attend(qkv_all[0], qkv_all[1], qkv_all[2])
        return (column_f + mod_rows[2] * out_proj(mixed_out, w_out_temporal)).astype(jnp.bfloat16)

    ctx_kv = qkv_proj(text_ctx, w_kv_cross)

    def cross_mlp_frame(frame_in):
        frame_f = frame_in.astype(jnp.float32)
        query_heads = qkv_proj(frame_in, w_query_cross[None])[0]
        mixed_out = attend(query_heads, ctx_kv[0], ctx_kv[1])
        after_cross = (frame_f + out_proj(mixed_out, w_out_cross)).astype(jnp.bfloat16)
        cross_f = after_cross.astype(jnp.float32)
        normed = (layer_norm(cross_f) * (1.0 + mod_rows[4]) + mod_rows[3]).astype(jnp.bfloat16)
        flat_rows = normed.reshape(-1, MODEL_WIDTH)
        mlp_hidden = jax.nn.gelu(jnp.dot(flat_rows, w_mlp_in, preferred_element_type=jnp.float32), approximate=True).astype(jnp.bfloat16)
        mlp_out = jnp.dot(mlp_hidden, w_mlp_out, preferred_element_type=jnp.float32).reshape(cross_f.shape)
        return (cross_f + mod_rows[5] * mlp_out).astype(jnp.bfloat16)

    after_spatial = lax.map(spatial_frame, jnp.moveaxis(latents, 1, 0))
    after_temporal = lax.map(temporal_patch, jnp.transpose(after_spatial, (2, 1, 0, 3)))
    out_frames = lax.map(cross_mlp_frame, jnp.transpose(after_temporal, (2, 1, 0, 3)))
    return jnp.moveaxis(out_frames, 0, 1)
```

```python
import functools

import jax
import jax.numpy as jnp
from jax import lax
from jax.experimental import pallas as pl
from jax.experimental.pallas import tpu as pltpu
from jax.sharding import PartitionSpec as P

LN_EPS = 1e-6
LOG2E = 1.4426950408889634
F32 = jnp.float32
BF16 = jnp.bfloat16
MESH = pl.DeviceIdType.MESH
WEIGHTS = ('w_qkv_s', 'w_out_s', 'w_qkv_t', 'w_out_t', 'w_q_c', 'w_kv_c', 'w_out_c', 'w_in', 'w_up')


def mm(lhs, rhs):
    return lax.dot_general(lhs, rhs, (((1,), (0,)), ((), ())), preferred_element_type=F32)


def mm_nt(lhs, rhs):
    return lax.dot_general(lhs, rhs, (((1,), (1,)), ((), ())), preferred_element_type=F32)


def mm_tn(lhs, rhs):
    return lax.dot_general(lhs, rhs, (((0,), (0,)), ((), ())), preferred_element_type=F32)


def layer_norm(acts):
    centered = acts - jnp.mean(acts, axis=-1, keepdims=True)
    return centered * lax.rsqrt(jnp.mean(centered * centered, axis=-1, keepdims=True) + LN_EPS)


def probs_t(scores_t, scale):
    shifted = (scores_t - jnp.max(scores_t, axis=0, keepdims=True)) * (scale * LOG2E)
    weights = jnp.exp2(shifted)
    return weights * (1.0 / jnp.sum(weights, axis=0, keepdims=True))


def padded_head(q_t, head, dim):
    rows = q_t[head * dim:(head + 1) * dim]
    zeros = jnp.zeros_like(rows)
    return jnp.concatenate([rows, zeros] if head % 2 == 0 else [zeros, rows], axis=0)


def head_pair(k, head, dim):
    lo = (head // 2) * 2 * dim
    return k[:, lo:lo + 2 * dim]


def project_qkv(acts, w_ref, width):
    q_t = mm_nt(w_ref[0:width], acts).astype(BF16)
    v_t = mm_nt(w_ref[2 * width:3 * width], acts).astype(BF16)
    k = mm_nt(acts, w_ref[width:2 * width]).astype(BF16)
    return q_t, k, v_t


def block_kernel(cfg, x_hbm, ctx_hbm, mod_hbm, pos_hbm, *rest):
    n, B, F, S, C, H, D, L = cfg
    PP = S // n
    T = F * n
    R = F * PP
    NW = len(WEIGHTS)
    w_hbm = rest[:NW]
    y_hbm = rest[NW]
    (xb, ctxb, modb, posb) = rest[NW + 1:NW + 5]
    wv = rest[NW + 5:2 * NW + 5]
    (sb1, rb1, sb2, rb2, zf, yb, kc, vc, lsem, xsem, ysem, ssem1, rsem1, ssem2, rsem2) = rest[2 * NW + 5:]
    w_qkv_s, w_out_s, w_qkv_t, w_out_t, w_q_c, w_kv_c, w_out_c, w_in, w_up = wv
    scale = D ** -0.5
    me = lax.axis_index('sp')

    def x_copy(b):
        return pltpu.make_async_copy(x_hbm.at[b], xb.at[b], xsem.at[b])

    loads = [pltpu.make_async_copy(src, dst, lsem.at[i]) for i, (src, dst) in enumerate(
        zip((ctx_hbm, mod_hbm, pos_hbm) + tuple(w_hbm), (ctxb, modb, posb) + tuple(wv)))]
    x_copy(0).start()
    loads[1].start()
    loads[3].start()
    loads[4].start()
    for b in range(1, B):
        x_copy(b).start()
    for i in (0, 2, 5, 6, 7, 8, 9, 10, 11):
        loads[i].start()

    barrier = pltpu.get_barrier_semaphore()

    @pl.loop(1, n)
    def _(j):
        pl.semaphore_signal(barrier, inc=1, device_id={'sp': lax.rem(me + j, n)}, device_id_type=MESH)

    pl.semaphore_wait(barrier, n - 1)

    def send_all(b, sbuf, rbuf, ssem, rsem):
        rbuf[b, me] = sbuf[b, me]

        @pl.loop(1, n)
        def _(j):
            peer = lax.rem(me + j, n)
            pltpu.make_async_remote_copy(
                src_ref=sbuf.at[b, peer], dst_ref=rbuf.at[b, me], send_sem=ssem.at[b], recv_sem=rsem.at[b],
                device_id={'sp': peer}, device_id_type=MESH).start()

    def whole(b, sbuf, rbuf, ssem, rsem):
        return pltpu.make_async_remote_copy(
            src_ref=sbuf.at[b, pl.ds(0, n - 1)], dst_ref=rbuf.at[b, pl.ds(0, n - 1)], send_sem=ssem.at[b],
            recv_sem=rsem.at[b], device_id={'sp': me}, device_id_type=MESH)

    loads[1].wait()
    loads[3].wait()
    loads[4].wait()

    @pl.loop(0, B)
    def _(b):
        x_copy(b).wait()
        mod = modb[b]
        outs = []
        for f in range(F):
            lat = xb[b, f].astype(F32)
            acts = (layer_norm(lat) * (1.0 + mod[1:2]) + mod[0:1]).astype(BF16)
            q_t, k, v_t = project_qkv(acts, w_qkv_s, C)
            heads = []
            for h in range(H):
                s_t = mm(head_pair(k, h, D), padded_head(q_t, h, D))
                p_t = probs_t(s_t, scale).astype(BF16)
                heads.append(mm(v_t[h * D:(h + 1) * D], p_t).astype(BF16))
            branch = mm_tn(jnp.concatenate(heads, axis=0), w_out_s[...])
            outs.append((lat + mod[2:3] * branch).reshape(n, PP, C))
        sb1[b] = jnp.concatenate(outs, axis=1).astype(BF16)
        send_all(b, sb1, rb1, ssem1, rsem1)

    loads[0].wait()
    loads[8].wait()

    @pl.loop(0, B)
    def _(b):
        ctx = ctxb[b]
        kc[b] = mm_nt(ctx, w_kv_c[0:C]).astype(BF16)
        vc[b] = mm_nt(ctx, w_kv_c[C:2 * C]).astype(BF16)

    loads[2].wait()
    loads[5].wait()
    loads[6].wait()
    group = 256 // T if T <= 128 else 1
    group = min(group, PP)

    @pl.loop(0, B)
    def _(b):
        whole(b, sb1, rb1, ssem1, rsem1).wait_recv()
        mod = modb[b]
        pos = posb[...]
        low = lax.broadcasted_iota(jnp.int32, (T, 2 * T), 1) < T
        arrived = rb1[b].astype(F32).reshape(n * R, C)
        for c in range(C // 128):
            zf[c] = arrived[:, c * 128:(c + 1) * 128]
        for g in range(PP // group):
            tokens = jnp.concatenate([jnp.concatenate(
                [zf[c, pl.ds(g * group + i, T, PP), :] for c in range(C // 128)], axis=1) for i in range(group)], axis=0)
            acts = (tokens + jnp.concatenate([pos] * group, axis=0)).astype(BF16)
            q_t, k, v_t = project_qkv(acts, w_qkv_t, C)
            heads = []
            for h in range(H):
                q_h = padded_head(q_t, h, D)
                k_h = head_pair(k, h, D)
                v_h = v_t[h * D:(h + 1) * D]
                parts = []
                for i in range(group // 2):
                    lanes = slice(i * 2 * T, (i + 1) * 2 * T)
                    s_t = mm(k_h[lanes], q_h[:, lanes])
                    p_t = probs_t(jnp.where(low, s_t[0:T], s_t[T:2 * T]), scale)
                    p_t = jnp.concatenate([jnp.where(low, p_t, 0.0), jnp.where(low, 0.0, p_t)], axis=0).astype(BF16)
                    parts.append(mm(v_h[:, lanes], p_t).astype(BF16))
                heads.append(jnp.concatenate(parts, axis=1))
            branch = mm_tn(jnp.concatenate(heads, axis=0), w_out_t[...])
            after = tokens + mod[2:3] * branch
            for i in range(group):
                for c in range(C // 128):
                    zf[c, pl.ds(g * group + i, T, PP), :] = after[i * T:(i + 1) * T, c * 128:(c + 1) * 128]
        leaving = jnp.concatenate([zf[c] for c in range(C // 128)], axis=1)
        sb2[b] = leaving.astype(BF16).reshape(n, R, C)
        send_all(b, sb2, rb2, ssem2, rsem2)

    for i in (7, 9, 10, 11):
        loads[i].wait()

    @pl.loop(0, B)
    def _(b):
        whole(b, sb2, rb2, ssem2, rsem2).wait_recv()
        mod = modb[b]
        k_all = kc[b]
        v_all = vc[b]
        for f in range(F):
            hid_f = rb2[b].astype(F32)[:, f * PP:(f + 1) * PP, :].reshape(S, C)
            q_t = mm_nt(w_q_c[...], hid_f.astype(BF16)).astype(BF16)
            heads = []
            for h in range(H):
                s_t = mm(head_pair(k_all, h, D), padded_head(q_t, h, D))
                p_t = probs_t(s_t, scale).astype(BF16)
                lo = (h // 2) * 2 * D
                o_t = mm_tn(v_all[:, lo:lo + 2 * D], p_t)
                heads.append(o_t[(h % 2) * D:(h % 2 + 1) * D].astype(BF16))
            branch = mm_tn(jnp.concatenate(heads, axis=0), w_out_c[...])
            cross = (hid_f + branch).astype(BF16).astype(F32)
            normed = (layer_norm(cross) * (1.0 + mod[4:5]) + mod[3:4]).astype(BF16)
            grown = jax.nn.gelu(mm(normed, w_in[...]), approximate=True).astype(BF16)
            yb[b, f] = (cross + mod[5:6] * mm(grown, w_up[...])).astype(BF16)
        pltpu.make_async_copy(yb.at[b], y_hbm.at[b], ysem.at[b]).start()

    @pl.loop(0, B)
    def _(b):
        pltpu.make_async_copy(yb.at[b], y_hbm.at[b], ysem.at[b]).wait()
        whole(b, sb1, rb1, ssem1, rsem1).wait_send()
        whole(b, sb2, rb2, ssem2, rsem2).wait_send()


def solution(mesh):
    n = mesh.shape['sp']
    act_spec = P('dp', 'sp', None, None)
    row_spec = P('dp', None, None)
    rep = [P(*[None] * k) for k in range(5)]
    in_specs = (act_spec, row_spec, row_spec, rep[2], rep[4], rep[3], rep[4], rep[3], rep[3], rep[4], rep[3], rep[2], rep[2])

    def local_block(latents, text_ctx, modulation, pos_temporal, w_qkv_spatial, w_out_spatial, w_qkv_temporal, w_out_temporal, w_query_cross, w_kv_cross, w_out_cross, w_mlp_in, w_mlp_out):
        B, F, S, C = latents.shape
        H, D, _ = w_out_spatial.shape
        L = text_ctx.shape[1]
        weights = [w.reshape(-1, w.shape[-1]) for w in (w_qkv_spatial, w_out_spatial, w_qkv_temporal, w_out_temporal, w_query_cross, w_kv_cross, w_out_cross, w_mlp_in, w_mlp_out)]
        args = [latents, text_ctx, modulation, pos_temporal] + weights
        R = F * (S // n)
        chunk = pltpu.VMEM((B, n, R, C), BF16)
        return pl.pallas_call(
            functools.partial(block_kernel, (n, B, F, S, C, H, D, L)),
            out_shape=jax.ShapeDtypeStruct(latents.shape, BF16),
            in_specs=[pl.BlockSpec(memory_space=pl.ANY)] * len(args),
            out_specs=pl.BlockSpec(memory_space=pl.ANY),
            scratch_shapes=[pltpu.VMEM(a.shape, a.dtype) for a in args] + [
                chunk, chunk, chunk, chunk,
                pltpu.VMEM((C // 128, n * R, 128), F32),
                pltpu.VMEM(latents.shape, BF16),
                pltpu.VMEM((B, L, C), BF16),
                pltpu.VMEM((B, L, C), BF16),
                pltpu.SemaphoreType.DMA((len(args) - 1,)),
                pltpu.SemaphoreType.DMA((B,)),
                pltpu.SemaphoreType.DMA((B,)),
                pltpu.SemaphoreType.DMA((B,)),
                pltpu.SemaphoreType.DMA((B,)),
                pltpu.SemaphoreType.DMA((B,)),
                pltpu.SemaphoreType.DMA((B,)),
            ],
            compiler_params=pltpu.CompilerParams(collective_id=0, has_side_effects=True, vmem_limit_bytes=60 * 1024 * 1024),
            name='st_block',
        )(*args)

    return jax.shard_map(local_block, mesh=mesh, in_specs=in_specs, out_specs=act_spec, check_vma=False)
```

```python
import functools

import jax
import jax.numpy as jnp
from jax import lax
from jax.experimental import pallas as pl
from jax.experimental.pallas import tpu as pltpu
from jax.sharding import PartitionSpec as P

LN_EPS = 1e-6
LOG2E = 1.4426950408889634
GELU_A = 0.7978845608028654
GELU_B = 0.044715 * GELU_A
F32 = jnp.float32
BF16 = jnp.bfloat16
MESH = pl.DeviceIdType.MESH
DEPTH = 4
WEIGHTS = ('w_qkv_s', 'w_out_s', 'w_qkv_t', 'w_out_t', 'w_q_c', 'w_kv_c', 'w_out_c', 'w_in', 'w_up')


def mm(lhs, rhs):
    return lax.dot_general(lhs, rhs, (((1,), (0,)), ((), ())), preferred_element_type=F32)


def mm_nt(lhs, rhs):
    return lax.dot_general(lhs, rhs, (((1,), (1,)), ((), ())), preferred_element_type=F32)


def mm_tn(lhs, rhs):
    return lax.dot_general(lhs, rhs, (((0,), (0,)), ((), ())), preferred_element_type=F32)


def gelu(acts):
    inner = acts * (GELU_A + GELU_B * (acts * acts))
    half = 0.5 * acts
    return half + half * jnp.tanh(inner)


def layer_norm(acts):
    centered = acts - jnp.mean(acts, axis=-1, keepdims=True)
    return centered * lax.rsqrt(jnp.mean(centered * centered, axis=-1, keepdims=True) + LN_EPS)


def padded_head(q_ref, head, dim, lanes):
    rows = q_ref[head * dim:(head + 1) * dim, lanes]
    zeros = jnp.zeros_like(rows)
    return jnp.concatenate([rows, zeros] if head % 2 == 0 else [zeros, rows], axis=0)


def pair_lanes(head, dim):
    lo = (head // 2) * 2 * dim
    return slice(lo, lo + 2 * dim)


def weights_t(scores_t, scale):
    top = jnp.max(scores_t, axis=0, keepdims=True)
    weights = jnp.exp2((scores_t - top) * (scale * LOG2E))
    return weights, 1.0 / jnp.sum(weights, axis=0, keepdims=True)


def staged(units, score, soften, combine):
    for i in range(len(units) + 2):
        if i < len(units):
            score(i % DEPTH, *units[i])
        if 0 <= i - 1 < len(units):
            soften((i - 1) % DEPTH, *units[i - 1])
        if 0 <= i - 2 < len(units):
            combine((i - 2) % DEPTH, *units[i - 2])


def block_kernel(cfg, x_hbm, ctx_hbm, mod_hbm, pos_hbm, *rest):
    n, B, F, S, C, H, D, L = cfg
    PP = S // n
    T = F * n
    R = F * PP
    NW = len(WEIGHTS)
    w_hbm = rest[:NW]
    y_hbm = rest[NW]
    (xb, ctxb, modb, posb) = rest[NW + 1:NW + 5]
    wv = rest[NW + 5:2 * NW + 5]
    (sb1, rb1, sb2, rb2, zf, yb, kc, vc, qs, ks, vs, at, sc, pc, rs, tok, act, grown, lsem, xsem, ysem, ssem1, rsem1, ssem2, rsem2) = rest[2 * NW + 5:]
    w_qkv_s, w_out_s, w_qkv_t, w_out_t, w_q_c, w_kv_c, w_out_c, w_in, w_up = wv
    scale = D ** -0.5
    me = lax.axis_index('sp')

    def x_copy(b):
        return pltpu.make_async_copy(x_hbm.at[b], xb.at[b], xsem.at[b])

    loads = [pltpu.make_async_copy(src, dst, lsem.at[i]) for i, (src, dst) in enumerate(
        zip((ctx_hbm, mod_hbm, pos_hbm) + tuple(w_hbm), (ctxb, modb, posb) + tuple(wv)))]
    x_copy(0).start()
    loads[1].start()
    loads[3].start()
    loads[4].start()
    for b in range(1, B):
        x_copy(b).start()
    for i in (0, 2, 5, 6, 7, 8, 9, 10, 11):
        loads[i].start()

    barrier = pltpu.get_barrier_semaphore()

    @pl.loop(1, n)
    def _(j):
        pl.semaphore_signal(barrier, inc=1, device_id={'sp': lax.rem(me + j, n)}, device_id_type=MESH)

    pl.semaphore_wait(barrier, n - 1)

    def send_all(b, sbuf, rbuf, ssem, rsem):
        rbuf[b, me] = sbuf[b, me]

        @pl.loop(1, n)
        def _(j):
            peer = lax.rem(me + j, n)
            pltpu.make_async_remote_copy(
                src_ref=sbuf.at[b, peer], dst_ref=rbuf.at[b, me], send_sem=ssem.at[b], recv_sem=rsem.at[b],
                device_id={'sp': peer}, device_id_type=MESH).start()

    def whole(b, sbuf, rbuf, ssem, rsem):
        return pltpu.make_async_remote_copy(
            src_ref=sbuf.at[b, pl.ds(0, n - 1)], dst_ref=rbuf.at[b, pl.ds(0, n - 1)], send_sem=ssem.at[b],
            recv_sem=rsem.at[b], device_id={'sp': me}, device_id_type=MESH)

    def project_qkv(i, w_ref):
        acts = act[i]
        qs[i] = mm_nt(w_ref[0:C], acts).astype(BF16)
        ks[i] = mm_nt(acts, w_ref[C:2 * C]).astype(BF16)
        vs[i] = mm_nt(w_ref[2 * C:3 * C], acts).astype(BF16)

    every = slice(None)

    loads[1].wait()
    loads[3].wait()
    loads[4].wait()

    def spatial_score(slot, f, h):
        sc[slot] = mm(ks[f, :, pair_lanes(h, D)], padded_head(qs.at[f], h, D, every))

    def spatial_soften(slot, f, h):
        weights, inverse = weights_t(sc[slot], scale)
        pc[slot] = weights.astype(BF16)
        rs[slot] = jnp.broadcast_to(inverse, rs.shape[1:])

    def spatial_combine(slot, f, h):
        mixed = mm(vs[f, h * D:(h + 1) * D], pc[slot]) * rs[slot, 0:1]
        at[h * D:(h + 1) * D, f * S:(f + 1) * S] = mixed.astype(BF16)

    units = [(f, h) for f in range(F) for h in range(H)]

    @pl.loop(0, B)
    def _(b):
        x_copy(b).wait()
        mod = modb[b]
        for f in range(F):
            act[f] = (layer_norm(xb[b, f].astype(F32)) * (1.0 + mod[1:2]) + mod[0:1]).astype(BF16)
            project_qkv(f, w_qkv_s)
        staged(units, spatial_score, spatial_soften, spatial_combine)
        branch = mm_tn(at[...], w_out_s[...])
        outs = [(xb[b, f].astype(F32) + mod[2:3] * branch[f * S:(f + 1) * S]).reshape(n, PP, C) for f in range(F)]
        sb1[b] = jnp.concatenate(outs, axis=1).astype(BF16)
        send_all(b, sb1, rb1, ssem1, rsem1)

    loads[0].wait()
    loads[8].wait()

    @pl.loop(0, B)
    def _(b):
        ctx = jnp.concatenate([ctxb[b].astype(F32), jnp.zeros((kc.shape[1] - L, C), F32)], axis=0).astype(BF16)
        kc[b] = mm_nt(ctx, w_kv_c[0:C]).astype(BF16)
        vc[b] = mm_nt(w_kv_c[C:2 * C], ctx).astype(BF16)

    loads[2].wait()
    loads[5].wait()
    loads[6].wait()
    G = S // T
    low = lax.broadcasted_iota(jnp.int32, (T, 2 * T), 1) < T
    pairs = [slice(i * 2 * T, (i + 1) * 2 * T) for i in range(G // 2)]

    def temporal_score(slot, g, h):
        for lanes in pairs:
            s_t = mm(ks[g, lanes, pair_lanes(h, D)], padded_head(qs.at[g], h, D, lanes))
            sc[slot, 0:T, lanes] = jnp.where(low, s_t[0:T], s_t[T:2 * T])

    def temporal_soften(slot, g, h):
        for lanes in pairs:
            weights, inverse = weights_t(sc[slot, 0:T, lanes], scale)
            pc[slot, 0:T, lanes] = jnp.where(low, weights, 0.0).astype(BF16)
            pc[slot, T:2 * T, lanes] = jnp.where(low, 0.0, weights).astype(BF16)
            rs[slot, :, lanes] = jnp.broadcast_to(inverse, (rs.shape[1], 2 * T))

    def temporal_combine(slot, g, h):
        for i, lanes in enumerate(pairs):
            mixed = mm(vs[g, h * D:(h + 1) * D, lanes], pc[slot, 0:2 * T, lanes]) * rs[slot, 0:1, lanes]
            at[h * D:(h + 1) * D, g * S + i * 2 * T:g * S + (i + 1) * 2 * T] = mixed.astype(BF16)

    groups = PP // G

    @pl.loop(0, B)
    def _(b):
        whole(b, sb1, rb1, ssem1, rsem1).wait_recv()
        mod = modb[b]
        arrived = rb1[b].astype(F32).reshape(n * R, C)
        for c in range(C // 128):
            zf[c] = arrived[:, c * 128:(c + 1) * 128]
        for g in range(groups):
            for i in range(G):
                rows = jnp.concatenate([zf[c, pl.ds(g * G + i, T, PP), :] for c in range(C // 128)], axis=1)
                tok[g, i * T:(i + 1) * T] = rows
                act[g, i * T:(i + 1) * T] = (rows + posb[...]).astype(BF16)
            project_qkv(g, w_qkv_t)
        staged([(g, h) for g in range(groups) for h in range(H)], temporal_score, temporal_soften, temporal_combine)
        branch = mm_tn(at[...], w_out_t[...])
        for g in range(groups):
            after = tok[g] + mod[2:3] * branch[g * S:(g + 1) * S]
            for i in range(G):
                for c in range(C // 128):
                    zf[c, pl.ds(g * G + i, T, PP), :] = after[i * T:(i + 1) * T, c * 128:(c + 1) * 128]
        leaving = jnp.concatenate([zf[c] for c in range(C // 128)], axis=1)
        sb2[b] = leaving.astype(BF16).reshape(n, R, C)
        send_all(b, sb2, rb2, ssem2, rsem2)

    for i in (7, 9, 10, 11):
        loads[i].wait()
    LP = kc.shape[1]

    @pl.loop(0, B)
    def _(b):
        whole(b, sb2, rb2, ssem2, rsem2).wait_recv()
        mod = modb[b]

        def cross_score(slot, f, h):
            sc[slot, 0:LP] = mm(kc[b, :, pair_lanes(h, D)], padded_head(qs.at[f], h, D, every))

        def cross_soften(slot, f, h):
            weights, inverse = weights_t(sc[slot, 0:L], scale)
            weights = jnp.concatenate([weights, jnp.zeros((LP - L, S), F32)], axis=0)
            pc[slot, 0:LP] = weights.astype(BF16)
            rs[slot] = jnp.broadcast_to(inverse, rs.shape[1:])

        def cross_combine(slot, f, h):
            mixed = mm(vc[b, h * D:(h + 1) * D], pc[slot, 0:LP]) * rs[slot, 0:1]
            at[h * D:(h + 1) * D, f * S:(f + 1) * S] = mixed.astype(BF16)

        hidden = rb2[b].astype(F32)
        for f in range(F):
            hid = hidden[:, f * PP:(f + 1) * PP, :].reshape(S, C)
            tok[f] = hid
            qs[f] = mm_nt(w_q_c[...], hid.astype(BF16)).astype(BF16)
        staged(units, cross_score, cross_soften, cross_combine)
        branch = mm_tn(at[...], w_out_c[...])
        for f in range(F):
            cross = (tok[f] + branch[f * S:(f + 1) * S]).astype(BF16).astype(F32)
            tok[f] = cross
            act[f] = (layer_norm(cross) * (1.0 + mod[4:5]) + mod[3:4]).astype(BF16)
        normed = act[...].reshape(F * S, C)
        wide = w_in.shape[1]
        for j in range(0, wide, 256):
            grown[:, j:j + 256] = gelu(mm(normed, w_in[:, j:j + 256])).astype(BF16)
        out = mm(grown[...], w_up[...])
        for f in range(F):
            yb[b, f] = (tok[f] + mod[5:6] * out[f * S:(f + 1) * S]).astype(BF16)
        pltpu.make_async_copy(yb.at[b], y_hbm.at[b], ysem.at[b]).start()

    @pl.loop(0, B)
    def _(b):
        pltpu.make_async_copy(yb.at[b], y_hbm.at[b], ysem.at[b]).wait()
        whole(b, sb1, rb1, ssem1, rsem1).wait_send()
        whole(b, sb2, rb2, ssem2, rsem2).wait_send()


def solution(mesh):
    n = mesh.shape['sp']
    act_spec = P('dp', 'sp', None, None)
    row_spec = P('dp', None, None)
    rep = [P(*[None] * k) for k in range(5)]
    in_specs = (act_spec, row_spec, row_spec, rep[2], rep[4], rep[3], rep[4], rep[3], rep[3], rep[4], rep[3], rep[2], rep[2])

    def local_block(latents, text_ctx, modulation, pos_temporal, w_qkv_spatial, w_out_spatial, w_qkv_temporal, w_out_temporal, w_query_cross, w_kv_cross, w_out_cross, w_mlp_in, w_mlp_out):
        B, F, S, C = latents.shape
        H, D, _ = w_out_spatial.shape
        L = text_ctx.shape[1]
        weights = [w.reshape(-1, w.shape[-1]) for w in (w_qkv_spatial, w_out_spatial, w_qkv_temporal, w_out_temporal, w_query_cross, w_kv_cross, w_out_cross, w_mlp_in, w_mlp_out)]
        args = [latents, text_ctx, modulation, pos_temporal] + weights
        R = F * (S // n)
        LP = -(-L // 16) * 16
        chunk = pltpu.VMEM((B, n, R, C), BF16)
        return pl.pallas_call(
            functools.partial(block_kernel, (n, B, F, S, C, H, D, L)),
            out_shape=jax.ShapeDtypeStruct(latents.shape, BF16),
            in_specs=[pl.BlockSpec(memory_space=pl.ANY)] * len(args),
            out_specs=pl.BlockSpec(memory_space=pl.ANY),
            scratch_shapes=[pltpu.VMEM(a.shape, a.dtype) for a in args] + [
                chunk, chunk, chunk, chunk,
                pltpu.VMEM((C // 128, n * R, 128), F32),
                pltpu.VMEM(latents.shape, BF16),
                pltpu.VMEM((B, LP, C), BF16),
                pltpu.VMEM((B, C, LP), BF16),
                pltpu.VMEM((F, C, S), BF16),
                pltpu.VMEM((F, S, C), BF16),
                pltpu.VMEM((F, C, S), BF16),
                pltpu.VMEM((C, F * S), BF16),
                pltpu.VMEM((DEPTH, S, S), F32),
                pltpu.VMEM((DEPTH, S, S), BF16),
                pltpu.VMEM((DEPTH, 8, S), F32),
                pltpu.VMEM((F, S, C), F32),
                pltpu.VMEM((F, S, C), BF16),
                pltpu.VMEM((F * S, w_mlp_in.shape[1]), BF16),
                pltpu.SemaphoreType.DMA((len(args) - 1,)),
                pltpu.SemaphoreType.DMA((B,)),
                pltpu.SemaphoreType.DMA((B,)),
                pltpu.SemaphoreType.DMA((B,)),
                pltpu.SemaphoreType.DMA((B,)),
                pltpu.SemaphoreType.DMA((B,)),
                pltpu.SemaphoreType.DMA((B,)),
            ],
            compiler_params=pltpu.CompilerParams(collective_id=0, has_side_effects=True, vmem_limit_bytes=60 * 1024 * 1024),
            name='st_block',
        )(*args)

    return jax.shard_map(local_block, mesh=mesh, in_specs=in_specs, out_specs=act_spec, check_vma=False)
```

```python
import functools

import jax
import jax.numpy as jnp
from jax import lax
from jax.experimental import pallas as pl
from jax.experimental.pallas import tpu as pltpu
from jax.sharding import PartitionSpec as P

LN_EPS = 1e-6
LOG2E = 1.4426950408889634
GELU_A = 0.7978845608028654
GELU_B = 0.044715 * GELU_A
F32 = jnp.float32
BF16 = jnp.bfloat16
MESH = pl.DeviceIdType.MESH
DEPTH = 4
VIDEOS = 2
WEIGHTS = ('w_qkv_s', 'w_out_s', 'w_qkv_t', 'w_out_t', 'w_q_c', 'w_kv_c', 'w_out_c', 'w_in', 'w_up')


def mm(lhs, rhs):
    return lax.dot_general(lhs, rhs, (((1,), (0,)), ((), ())), preferred_element_type=F32)


def mm_nt(lhs, rhs):
    return lax.dot_general(lhs, rhs, (((1,), (1,)), ((), ())), preferred_element_type=F32)


def mm_tn(lhs, rhs):
    return lax.dot_general(lhs, rhs, (((0,), (0,)), ((), ())), preferred_element_type=F32)


def gelu(acts):
    inner = acts * (GELU_A + GELU_B * (acts * acts))
    half = 0.5 * acts
    return half + half * jnp.tanh(inner)


def layer_norm(acts):
    centered = acts - jnp.mean(acts, axis=-1, keepdims=True)
    return centered * lax.rsqrt(jnp.mean(centered * centered, axis=-1, keepdims=True) + LN_EPS)


def padded_head(q_ref, head, dim, lanes):
    rows = q_ref[head * dim:(head + 1) * dim, lanes]
    zeros = jnp.zeros_like(rows)
    return jnp.concatenate([rows, zeros] if head % 2 == 0 else [zeros, rows], axis=0)


def pair_lanes(head, dim):
    lo = (head // 2) * 2 * dim
    return slice(lo, lo + 2 * dim)


def weights_t(scores_t, scale):
    top = jnp.max(scores_t, axis=0, keepdims=True)
    weights = jnp.exp2((scores_t - top) * (scale * LOG2E))
    return weights, 1.0 / jnp.sum(weights, axis=0, keepdims=True)


def staged(units, score, soften, combine):
    for i in range(len(units) + 2):
        if i < len(units):
            score(i % DEPTH, *units[i])
        if 0 <= i - 1 < len(units):
            soften((i - 1) % DEPTH, *units[i - 1])
        if 0 <= i - 2 < len(units):
            combine((i - 2) % DEPTH, *units[i - 2])


def send_order(n):
    side = max(k for k in range(1, n) if (n // 2) % k == 0 and k * k <= n // 2)
    rows = n // 2 // side
    lists = []
    for turn, dx in enumerate([1 % side, side - 1] + [k for k in range(side) if k not in (1 % side, side - 1)]):
        steps = [(dy + turn) % rows for dy in range(rows)]
        lists.append([(dy, dx, dc) for dc in range(2) for dy in steps])
    if side == 1:
        lists = lists[:1]
    longest = max(len(part) for part in lists)
    order = [part[i] for i in range(longest) for part in lists if i < len(part)]
    order = list(dict.fromkeys(order))
    return side, [offset for offset in order if offset != (0, 0, 0)]


def block_kernel(cfg, x_hbm, ctx_hbm, mod_hbm, pos_hbm, *rest):
    n, B, F, S, C, H, D, L = cfg
    PP = S // n
    T = F * n
    V = VIDEOS if B % VIDEOS == 0 else 1
    R = F * PP
    NW = len(WEIGHTS)
    w_hbm = rest[:NW]
    y_hbm = rest[NW]
    (xb, ctxb, modb, posb) = rest[NW + 1:NW + 5]
    wv = rest[NW + 5:2 * NW + 5]
    (sb1, rb1, sb2, rb2, zf, yb, kc, vc, qs, ks, vs, at, sc, pc, rs, tok, act, grown, lsem, xsem, ysem, ssem1, rsem1, ssem2, rsem2) = rest[2 * NW + 5:]
    w_qkv_s, w_out_s, w_qkv_t, w_out_t, w_q_c, w_kv_c, w_out_c, w_in, w_up = wv
    scale = D ** -0.5
    me = lax.axis_index('sp')
    side, order = send_order(n)

    def peer_of(offset):
        dy, dx, dc = offset
        x = lax.rem(me // 2, side)
        y = me // (2 * side)
        return (lax.rem(y + dy, n // (2 * side)) * side + lax.rem(x + dx, side)) * 2 + lax.rem(me + dc, 2)


    def x_copy(b):
        return pltpu.make_async_copy(x_hbm.at[b], xb.at[b], xsem.at[b])

    loads = [pltpu.make_async_copy(src, dst, lsem.at[i]) for i, (src, dst) in enumerate(
        zip((ctx_hbm, mod_hbm, pos_hbm) + tuple(w_hbm), (ctxb, modb, posb) + tuple(wv)))]
    x_copy(0).start()
    loads[1].start()
    loads[3].start()
    loads[4].start()
    for b in range(1, B):
        x_copy(b).start()
    for i in (0, 2, 5, 6, 7, 8, 9, 10, 11):
        loads[i].start()

    barrier = pltpu.get_barrier_semaphore()

    @pl.loop(1, n)
    def _(j):
        pl.semaphore_signal(barrier, inc=1, device_id={'sp': lax.rem(me + j, n)}, device_id_type=MESH)

    def send_all(g, sbuf, rbuf, ssem, rsem):
        rbuf[g, me] = sbuf[g, me]
        for offset in order:
            peer = peer_of(offset)
            pltpu.make_async_remote_copy(
                src_ref=sbuf.at[g, peer], dst_ref=rbuf.at[g, me], send_sem=ssem.at[g], recv_sem=rsem.at[g],
                device_id={'sp': peer}, device_id_type=MESH).start()

    def whole(g, sbuf, rbuf, ssem, rsem):
        return pltpu.make_async_remote_copy(
            src_ref=sbuf.at[g, pl.ds(0, n - 1)], dst_ref=rbuf.at[g, pl.ds(0, n - 1)], send_sem=ssem.at[g],
            recv_sem=rsem.at[g], device_id={'sp': me}, device_id_type=MESH)

    def project_qkv(i, w_ref):
        acts = act[i]
        qs[i] = mm_nt(w_ref[0:C], acts).astype(BF16)
        ks[i] = mm_nt(acts, w_ref[C:2 * C]).astype(BF16)
        vs[i] = mm_nt(w_ref[2 * C:3 * C], acts).astype(BF16)

    every = slice(None)

    loads[1].wait()
    loads[3].wait()
    loads[4].wait()

    def spatial_score(slot, f, h):
        sc[slot] = mm(ks[f, :, pair_lanes(h, D)], padded_head(qs.at[f], h, D, every))

    def spatial_soften(slot, f, h):
        weights, inverse = weights_t(sc[slot], scale)
        pc[slot] = weights.astype(BF16)
        rs[slot] = jnp.broadcast_to(inverse, rs.shape[1:])

    def spatial_combine(slot, f, h):
        mixed = mm(vs[f, h * D:(h + 1) * D], pc[slot]) * rs[slot, 0:1]
        at[h * D:(h + 1) * D, f * S:(f + 1) * S] = mixed.astype(BF16)

    units = [(f, h) for f in range(F) for h in range(H)]

    def spatial(g, i):
        b = g * V + i
        x_copy(b).wait()
        mod = modb[b]
        for f in range(F):
            act[f] = (layer_norm(xb[b, f].astype(F32)) * (1.0 + mod[1:2]) + mod[0:1]).astype(BF16)
            project_qkv(f, w_qkv_s)
        staged(units, spatial_score, spatial_soften, spatial_combine)
        branch = mm_tn(at[...], w_out_s[...])
        outs = [(xb[b, f].astype(F32) + mod[2:3] * branch[f * S:(f + 1) * S]).reshape(n, PP, C) for f in range(F)]
        sb1[g, :, i] = jnp.concatenate(outs, axis=1).astype(BF16)

    @pl.loop(0, B // V)
    def _(g):
        pl.loop(0, V)(functools.partial(spatial, g))

        @pl.when(g == 0)
        def _():
            pl.semaphore_wait(barrier, n - 1)

        send_all(g, sb1, rb1, ssem1, rsem1)

    loads[0].wait()
    loads[8].wait()

    @pl.loop(0, B)
    def _(b):
        ctx = jnp.concatenate([ctxb[b].astype(F32), jnp.zeros((kc.shape[1] - L, C), F32)], axis=0).astype(BF16)
        kc[b] = mm_nt(ctx, w_kv_c[0:C]).astype(BF16)
        vc[b] = mm_nt(w_kv_c[C:2 * C], ctx).astype(BF16)

    loads[2].wait()
    loads[5].wait()
    loads[6].wait()
    G = S // T
    low = lax.broadcasted_iota(jnp.int32, (T, 2 * T), 1) < T
    pairs = [slice(i * 2 * T, (i + 1) * 2 * T) for i in range(G // 2)]

    def temporal_score(slot, g, h):
        for lanes in pairs:
            s_t = mm(ks[g, lanes, pair_lanes(h, D)], padded_head(qs.at[g], h, D, lanes))
            sc[slot, 0:T, lanes] = jnp.where(low, s_t[0:T], s_t[T:2 * T])

    def temporal_soften(slot, g, h):
        for lanes in pairs:
            weights, inverse = weights_t(sc[slot, 0:T, lanes], scale)
            pc[slot, 0:T, lanes] = jnp.where(low, weights, 0.0).astype(BF16)
            pc[slot, T:2 * T, lanes] = jnp.where(low, 0.0, weights).astype(BF16)
            rs[slot, :, lanes] = jnp.broadcast_to(inverse, (rs.shape[1], 2 * T))

    def temporal_combine(slot, g, h):
        for i, lanes in enumerate(pairs):
            mixed = mm(vs[g, h * D:(h + 1) * D, lanes], pc[slot, 0:2 * T, lanes]) * rs[slot, 0:1, lanes]
            at[h * D:(h + 1) * D, g * S + i * 2 * T:g * S + (i + 1) * 2 * T] = mixed.astype(BF16)

    groups = PP // G

    def temporal(grp, vid):
        b = grp * V + vid
        mod = modb[b]
        arrived = rb1[grp, :, vid].astype(F32).reshape(n * R, C)
        for c in range(C // 128):
            zf[c] = arrived[:, c * 128:(c + 1) * 128]
        for g in range(groups):
            for i in range(G):
                rows = jnp.concatenate([zf[c, pl.ds(g * G + i, T, PP), :] for c in range(C // 128)], axis=1)
                tok[g, i * T:(i + 1) * T] = rows
                act[g, i * T:(i + 1) * T] = (rows + posb[...]).astype(BF16)
            project_qkv(g, w_qkv_t)
        staged([(g, h) for g in range(groups) for h in range(H)], temporal_score, temporal_soften, temporal_combine)
        branch = mm_tn(at[...], w_out_t[...])
        for g in range(groups):
            after = tok[g] + mod[2:3] * branch[g * S:(g + 1) * S]
            for i in range(G):
                for c in range(C // 128):
                    zf[c, pl.ds(g * G + i, T, PP), :] = after[i * T:(i + 1) * T, c * 128:(c + 1) * 128]
        leaving = jnp.concatenate([zf[c] for c in range(C // 128)], axis=1)
        sb2[grp, :, vid] = leaving.astype(BF16).reshape(n, R, C)

    @pl.loop(0, B // V)
    def _(grp):
        whole(grp, sb1, rb1, ssem1, rsem1).wait_recv()
        pl.loop(0, V)(functools.partial(temporal, grp))
        send_all(grp, sb2, rb2, ssem2, rsem2)

    for i in (7, 9, 10, 11):
        loads[i].wait()
    LP = kc.shape[1]

    def final(grp, vid):
        b = grp * V + vid
        mod = modb[b]

        def cross_score(slot, f, h):
            sc[slot, 0:LP] = mm(kc[b, :, pair_lanes(h, D)], padded_head(qs.at[f], h, D, every))

        def cross_soften(slot, f, h):
            weights, inverse = weights_t(sc[slot, 0:L], scale)
            weights = jnp.concatenate([weights, jnp.zeros((LP - L, S), F32)], axis=0)
            pc[slot, 0:LP] = weights.astype(BF16)
            rs[slot] = jnp.broadcast_to(inverse, rs.shape[1:])

        def cross_combine(slot, f, h):
            mixed = mm(vc[b, h * D:(h + 1) * D], pc[slot, 0:LP]) * rs[slot, 0:1]
            at[h * D:(h + 1) * D, f * S:(f + 1) * S] = mixed.astype(BF16)

        hidden = rb2[grp, :, vid].astype(F32)
        for f in range(F):
            hid = hidden[:, f * PP:(f + 1) * PP, :].reshape(S, C)
            tok[f] = hid
            qs[f] = mm_nt(w_q_c[...], hid.astype(BF16)).astype(BF16)
        staged(units, cross_score, cross_soften, cross_combine)
        branch = mm_tn(at[...], w_out_c[...])
        for f in range(F):
            cross = (tok[f] + branch[f * S:(f + 1) * S]).astype(BF16).astype(F32)
            tok[f] = cross
            act[f] = (layer_norm(cross) * (1.0 + mod[4:5]) + mod[3:4]).astype(BF16)
        normed = act[...].reshape(F * S, C)
        wide = w_in.shape[1]
        for j in range(0, wide, 256):
            grown[:, j:j + 256] = gelu(mm(normed, w_in[:, j:j + 256])).astype(BF16)
        out = mm(grown[...], w_up[...])
        for f in range(F):
            yb[b, f] = (tok[f] + mod[5:6] * out[f * S:(f + 1) * S]).astype(BF16)
        pltpu.make_async_copy(yb.at[b], y_hbm.at[b], ysem.at[b]).start()

    @pl.loop(0, B // V)
    def _(grp):
        whole(grp, sb2, rb2, ssem2, rsem2).wait_recv()
        pl.loop(0, V)(functools.partial(final, grp))

    @pl.loop(0, B)
    def _(b):
        pltpu.make_async_copy(yb.at[b], y_hbm.at[b], ysem.at[b]).wait()

    @pl.loop(0, B // V)
    def _(g):
        whole(g, sb1, rb1, ssem1, rsem1).wait_send()
        whole(g, sb2, rb2, ssem2, rsem2).wait_send()


def solution(mesh):
    n = mesh.shape['sp']
    act_spec = P('dp', 'sp', None, None)
    row_spec = P('dp', None, None)
    rep = [P(*[None] * k) for k in range(5)]
    in_specs = (act_spec, row_spec, row_spec, rep[2], rep[4], rep[3], rep[4], rep[3], rep[3], rep[4], rep[3], rep[2], rep[2])

    def local_block(latents, text_ctx, modulation, pos_temporal, w_qkv_spatial, w_out_spatial, w_qkv_temporal, w_out_temporal, w_query_cross, w_kv_cross, w_out_cross, w_mlp_in, w_mlp_out):
        B, F, S, C = latents.shape
        H, D, _ = w_out_spatial.shape
        L = text_ctx.shape[1]
        weights = [w.reshape(-1, w.shape[-1]) for w in (w_qkv_spatial, w_out_spatial, w_qkv_temporal, w_out_temporal, w_query_cross, w_kv_cross, w_out_cross, w_mlp_in, w_mlp_out)]
        args = [latents, text_ctx, modulation, pos_temporal] + weights
        R = F * (S // n)
        LP = -(-L // 16) * 16
        V = VIDEOS if B % VIDEOS == 0 else 1
        chunk = pltpu.VMEM((B // V, n, V, R, C), BF16)
        return pl.pallas_call(
            functools.partial(block_kernel, (n, B, F, S, C, H, D, L)),
            out_shape=jax.ShapeDtypeStruct(latents.shape, BF16),
            in_specs=[pl.BlockSpec(memory_space=pl.ANY)] * len(args),
            out_specs=pl.BlockSpec(memory_space=pl.ANY),
            scratch_shapes=[pltpu.VMEM(a.shape, a.dtype) for a in args] + [
                chunk, chunk, chunk, chunk,
                pltpu.VMEM((C // 128, n * R, 128), F32),
                pltpu.VMEM(latents.shape, BF16),
                pltpu.VMEM((B, LP, C), BF16),
                pltpu.VMEM((B, C, LP), BF16),
                pltpu.VMEM((F, C, S), BF16),
                pltpu.VMEM((F, S, C), BF16),
                pltpu.VMEM((F, C, S), BF16),
                pltpu.VMEM((C, F * S), BF16),
                pltpu.VMEM((DEPTH, S, S), F32),
                pltpu.VMEM((DEPTH, S, S), BF16),
                pltpu.VMEM((DEPTH, 8, S), F32),
                pltpu.VMEM((F, S, C), F32),
                pltpu.VMEM((F, S, C), BF16),
                pltpu.VMEM((F * S, w_mlp_in.shape[1]), BF16),
                pltpu.SemaphoreType.DMA((len(args) - 1,)),
                pltpu.SemaphoreType.DMA((B,)),
                pltpu.SemaphoreType.DMA((B,)),
                pltpu.SemaphoreType.DMA((B // V,)),
                pltpu.SemaphoreType.DMA((B // V,)),
                pltpu.SemaphoreType.DMA((B // V,)),
                pltpu.SemaphoreType.DMA((B // V,)),
            ],
            compiler_params=pltpu.CompilerParams(collective_id=0, has_side_effects=True, vmem_limit_bytes=60 * 1024 * 1024),
            name='st_block',
        )(*args)

    return jax.shard_map(local_block, mesh=mesh, in_specs=in_specs, out_specs=act_spec, check_vma=False)
```
